32 devices in a mesh: space: 8 (over y, x, core), mode: 4 (over z).
Axes of the slice: x: 2, y: 2, z: 4, core: 2. Of those that a mesh axis runs over, the one named last changes fastest.
Arguments:
- test_modes: float32 [32, 3, 8, 16, 256], P(None, None, None, 'space'), may hold values from -6 to 6
- modes: float32 [128, 3, 8, 16, 256], P('mode', None, None, 'space'), may hold values from -6 to 6
Outputs:
- triad: float32 [32, 128, 128], P('space', 'mode')
The draws below stay inside these ranges and needn't reach their ends.
All inputs are finite; a program needn't handle non-finite values.
Results may differ from the reference program's by a relative error of at most 0.000071.
Values sent between devices are 32-bit elements; how exact they have to be, the bound alone decides.
No kernel may reach another device: no remote copies, remote signals or barrier semaphores. Data moves between devices by JAX's collectives and lax.ppermute only.
A program may use at most 64 MiB of HBM per device.

```python
import math
import jax
import jax.numpy as jnp
from jax import lax

MODES = 128
I_BLK = 32
NX = 256
NZ = 8
NY = 16


def levels(own_key, shape, split, least, high):
    loudness, own = 1.0, jax.random.fold_in(own_key, 6)
    for position, blocks in split:
        steps = jnp.exp(jax.random.uniform(jax.random.fold_in(own, position), (blocks,), jnp.float32, least / len(split), high / len(split)))
        loudness = loudness * jnp.repeat(steps, shape[position] // blocks).reshape([-1 if axis == position else 1 for axis in range(len(shape))])
    return loudness


def bell_draw(own_key, dims, scale, bound, cuts=(), kind=jnp.bfloat16):
    drawn = scale * jax.random.normal(own_key, dims, jnp.float32)
    if cuts:
        drawn = drawn * levels(own_key, dims, cuts, -0.22, 0.18)
    return jnp.clip(drawn, -bound, bound).astype(kind)


def setup_inputs(seed: int = 0) -> dict:
    key_of = jax.random.split(jax.random.key(seed), 3)
    return {
        "test_modes": bell_draw(key_of[0], (I_BLK, 3, NZ, NY, NX), 1.0, 6.0, ((3, 8),), jnp.float32),
        "modes": bell_draw(key_of[1], (MODES, 3, NZ, NY, NX), 1.0, 6.0, ((0, 4), (3, 8)), jnp.float32),
    }


def central_diff(field, along):
    ahead = jnp.roll(field, -1, along) - jnp.roll(field, 1, along)
    farther = jnp.roll(field, -2, along) - jnp.roll(field, 2, along)
    return (8.0 * ahead - farther) / 12.0

def reference(test_modes, modes):
    volume_scale = 1.0 / math.sqrt(NX * NY * NZ)
    test_flat = test_modes.reshape(I_BLK, 3, -1)
    mode_flat = modes.reshape(MODES, 3, -1)

    def one_mode(field):
        gradients = jnp.stack([central_diff(field, 3), central_diff(field, 2), central_diff(field, 1)], axis=1)
        gradients = gradients.reshape(3, 3, -1)
        weighted = test_flat[:, 0, None, :] * gradients[0][None]
        weighted = weighted + test_flat[:, 1, None, :] * gradients[1][None]
        weighted = weighted + test_flat[:, 2, None, :] * gradients[2][None]
        return jnp.einsum('ibc,jbc->ij', weighted, mode_flat, precision=lax.Precision.HIGHEST)
    stacked = lax.map(one_mode, modes)
    return jnp.transpose(stacked, (1, 0, 2)) * volume_scale
```

```python
import math
from functools import partial

import jax
import jax.numpy as jnp
from jax import lax
from jax.experimental import pallas as pl
from jax.experimental.pallas import tpu as pltpu
from jax.sharding import PartitionSpec as P

LANES = 128
PITCH_PAD = 8


def flat_rows(field):
    count, comps, nz, rows, nx = field.shape
    tiles = nx // LANES
    split = field.reshape(count, comps, nz, rows, tiles, LANES)
    return split.transpose(0, 1, 2, 4, 3, 5).reshape(count, comps * nz * tiles * rows, LANES)


def lane_ids(count):
    return lax.broadcasted_iota(jnp.int32, (count, LANES), 1)


def chunk_kernel(dims, shifts, halos, me_ref, src_ref, *refs):
    count, nz, rows, nx, chunk, parts = dims
    tiles = nx // LANES
    outs, scratch, sem = refs[:-2], refs[-2], refs[-1]
    depth = 3 * nz * tiles * rows
    pitch = depth + PITCH_PAD
    copy = pltpu.make_async_copy(src_ref, scratch.reshape(count, pitch, LANES).at[:, pl.ds(0, depth), :], sem)
    copy.start()
    copy.wait()
    lane = lane_ids(count)

    def load(a, z, tile, y):
        return scratch[pl.ds(((a * nz + z) * tiles + tile) * rows + y, count, stride=pitch), :]

    def moved(value, amount):
        return pltpu.roll(value, lax.rem(amount + 2 * LANES, LANES), 1)

    for index, shift in enumerate(shifts):
        part = lax.rem(me_ref[0] + shift, parts)
        start = part * chunk
        left = lax.rem(start + nx - 2, nx)
        right = lax.rem(start + chunk, nx)
        field_out = outs[index]
        for a in range(3):
            packed = jnp.zeros((count, LANES), jnp.float32)
            for z in range(nz):
                value = jnp.zeros((count, LANES), jnp.float32)
                for y in range(rows):
                    row = moved(load(a, z, start // LANES, y), y * chunk - lax.rem(start, LANES))
                    mine = (lane >= y * chunk) & (lane < (y + 1) * chunk)
                    value = jnp.where(mine, row, value)
                    if halos:
                        at = y * chunk + 2 * z
                        low = moved(load(a, z, left // LANES, y), at - lax.rem(left, LANES))
                        packed = jnp.where((lane >= at) & (lane < at + 2), low, packed)
                        at = (y + 1) * chunk - 2 - 2 * z
                        high = moved(load(a, z, right // LANES, y), at - lax.rem(right, LANES))
                        packed = jnp.where((lane >= at) & (lane < at + 2), high, packed)
                field_out[z, a] = value
            if halos:
                field_out[nz, a] = packed


def chunks(field, me, parts, shifts, halos):
    count, comps, nz, rows, nx = field.shape
    chunk = nx // parts
    flat = flat_rows(field)
    dims = (count, nz, rows, nx, chunk, parts)
    shape = (nz + 1 if halos else nz, comps, count, LANES)
    return pl.pallas_call(
        partial(chunk_kernel, dims, shifts, halos),
        out_shape=[jax.ShapeDtypeStruct(shape, jnp.float32) for _ in shifts],
        in_specs=[pl.BlockSpec(memory_space=pltpu.SMEM), pl.BlockSpec(memory_space=pl.ANY)],
        scratch_shapes=[
            pltpu.VMEM((count * (flat.shape[1] + PITCH_PAD), LANES), jnp.float32),
            pltpu.SemaphoreType.DMA,
        ],
        name="chunks",
    )(me, flat)


def split_pair(value):
    high = value.astype(jnp.bfloat16)
    return high, (value - high.astype(jnp.float32)).astype(jnp.bfloat16)


def put_right(right_ref, unit, z, at, total, value):
    high, low = split_pair(value)
    count = value.shape[0]
    right_ref[unit, pl.ds(at, count), pl.ds(z * LANES, LANES)] = high
    right_ref[unit, pl.ds(total + at, count), pl.ds(z * LANES, LANES)] = low


def contract(units, nz, group, total, test_refs, grad_ref, right_ref, high_ref, low_ref):
    first = pl.program_id(0) * group
    for unit in range(units):
        for z in range(nz):
            tests = [[test_refs[unit][z, a, pl.ds(first + i, 1), :] for a in range(3)] for i in range(group)]
            grads = [grad_ref[(unit * 3 + a) * nz + z] for a in range(3)]
            for i in range(group):
                weighted = tests[i][0] * grads[0] + tests[i][1] * grads[1] + tests[i][2] * grads[2]
                high, low = split_pair(weighted)
                where = (pl.ds(i * total, total), pl.ds((unit * nz + z) * LANES, LANES))
                high_ref[where] = high
                low_ref[where] = low
    result = None
    for unit in range(units):
        span = pl.ds(unit * nz * LANES, nz * LANES)
        dims = (((1,), (1,)), ((), ()))
        both = lax.dot_general(high_ref[:, span], right_ref[unit], dims, preferred_element_type=jnp.float32)
        low = lax.dot_general(low_ref[:, span], right_ref[unit, :total], dims, preferred_element_type=jnp.float32)
        part = both[:, :total] + both[:, total:] + low
        result = part if result is None else result + part
    return result


def xz_kernel(dims, me_ref, test_ref, *refs):
    parts, count, nz, chunk, group = dims
    total = parts * count
    fields, (out_ref, grad_ref, right_ref, high_ref, low_ref) = refs[:parts], refs[parts:]

    @pl.when(pl.program_id(0) == 0)
    def _():
        lane = lane_ids(count)
        place = lax.rem(lane, chunk)
        for shift in range(parts):
            field = fields[shift]
            at = pl.multiple_of(lax.rem(me_ref[0] + parts - shift, parts) * count, count)

            def one_comp(a, carry):
                packed = field[nz, a]
                for z in range(nz):
                    value = field[z, a]
                    edge = jnp.where(place < 2, pltpu.roll(packed, (LANES - 2 * z) % LANES, 1), pltpu.roll(packed, 2 * z, 1))
                    up = jnp.where(place == chunk - 1, pltpu.roll(edge, 1, 1), pltpu.roll(value, LANES - 1, 1))
                    down = jnp.where(place == 0, pltpu.roll(edge, LANES - 1, 1), pltpu.roll(value, 1, 1))
                    up2 = jnp.where(place >= chunk - 2, edge, pltpu.roll(value, LANES - 2, 1))
                    down2 = jnp.where(place < 2, edge, pltpu.roll(value, 2, 1))
                    grad_ref[a * nz + z, pl.ds(at, count), :] = 8.0 * (up - down) - (up2 - down2)
                    ahead = field[(z + 1) % nz, a] - field[(z - 1) % nz, a]
                    farther = field[(z + 2) % nz, a] - field[(z - 2) % nz, a]
                    grad_ref[(3 + a) * nz + z, pl.ds(at, count), :] = 8.0 * ahead - farther
                return carry

            lax.fori_loop(0, 3, one_comp, 0)
            for z in range(nz):
                put_right(right_ref, 0, z, at, total, field[z, 0])
                put_right(right_ref, 1, z, at, total, field[z, 2])

    out_ref[...] = contract(2, nz, group, total, (test_ref, test_ref), grad_ref, right_ref, high_ref, low_ref)


def y_kernel(dims, me_ref, test_ref, next_test_ref, run_ref, *refs):
    parts, count, nz, chunk, group, scale = dims
    total = parts * count
    fields, nexts = refs[:parts], refs[parts : 2 * parts]
    out_ref, grad_ref, right_ref, high_ref, low_ref = refs[2 * parts :]

    @pl.when(pl.program_id(0) == 0)
    def _():
        lane = lane_ids(count)
        first = lane < chunk

        def swapped(value):
            if 2 * chunk == LANES:
                return pltpu.roll(value, chunk, 1)
            return jnp.where(first, pltpu.roll(value, LANES - chunk, 1), pltpu.roll(value, chunk, 1))

        for shift in range(parts):
            field, following = fields[shift], nexts[shift]
            at = pl.multiple_of(lax.rem(me_ref[0] + parts - shift, parts) * count, count)

            def one_comp(a, carry):
                for z in range(nz):
                    own, ahead = field[z, a], following[z, a]
                    turned = 8.0 * swapped(own)
                    mine = jnp.where(first, turned, 8.0 * swapped(ahead) - turned) - ahead
                    theirs = own - jnp.where(first, turned, 0.0)
                    grad_ref[a * nz + z, pl.ds(at, count), :] = mine
                    grad_ref[(3 + a) * nz + z, pl.ds(at, count), :] = theirs
                return carry

            lax.fori_loop(0, 3, one_comp, 0)
            for z in range(nz):
                put_right(right_ref, 0, z, at, total, field[z, 1])
                put_right(right_ref, 1, z, at, total, following[z, 1])

    part = contract(2, nz, group, total, (test_ref, next_test_ref), grad_ref, right_ref, high_ref, low_ref)
    out_ref[...] = (run_ref[...] + part) * scale


def part_call(kernel, name, me, whole, running, parts, count, nz, tests, group):
    total = parts * count
    keep = lambda value: pl.BlockSpec(value.shape, lambda g, nd=value.ndim: (0,) * nd, pipeline_mode=pl.Buffered(1))
    rows = pl.BlockSpec((group * total, total), lambda g: (g, 0))
    return pl.pallas_call(
        kernel,
        grid=(tests // group,),
        out_shape=jax.ShapeDtypeStruct((tests * total, total), jnp.float32),
        in_specs=[pl.BlockSpec(memory_space=pltpu.SMEM)]
        + [rows if value is running else keep(value) for value in whole],
        out_specs=rows,
        scratch_shapes=[
            pltpu.VMEM((6 * nz, total, LANES), jnp.float32),
            pltpu.VMEM((2, 2 * total, nz * LANES), jnp.bfloat16),
            pltpu.VMEM((group * total, 2 * nz * LANES), jnp.bfloat16),
            pltpu.VMEM((group * total, 2 * nz * LANES), jnp.bfloat16),
        ],
        compiler_params=pltpu.CompilerParams(dimension_semantics=("arbitrary",)),
        cost_estimate=pl.CostEstimate(flops=2 * 6 * nz * LANES * tests * total * total, transcendentals=0, bytes_accessed=8 * tests * total * total),
        name=name,
    )(me, *whole)


def shifted(value, axis, shift):
    size = lax.axis_size(axis)
    return lax.ppermute(value, axis, [(i, (i + shift) % size) for i in range(size)])


def scattered(value, axis, dim):
    size, me = lax.axis_size(axis), lax.axis_index(axis)
    length = value.shape[dim] // size
    total = lax.dynamic_slice_in_dim(value, me * length, length, dim)
    for shift in range(1, size):
        block = lax.dynamic_slice_in_dim(value, lax.rem(me + shift, size) * length, length, dim)
        total = total + shifted(block, axis, shift)
    return total


def per_device(test_modes, modes):
    count, comps, nz, rows, nx = modes.shape
    tests = test_modes.shape[0]
    parts = lax.axis_size("mode")
    total = parts * count
    chunk = nx // parts
    assert rows == 2 and rows * chunk <= LANES
    group = 4
    me = lax.axis_index("mode").astype(jnp.int32).reshape(1)
    scale = 1.0 / (12.0 * math.sqrt(nx * nz * rows * lax.axis_size("space")))

    sends = chunks(modes, me, parts, tuple(range(parts)), True)
    test = chunks(test_modes, me, parts, (0,), False)[0]
    next_test = shifted(test, "space", -1)
    fields = [sends[0]] + [shifted(sends[shift], "mode", shift) for shift in range(1, parts)]
    nexts = [shifted(field[:nz], "space", -1) for field in fields]

    running = part_call(
        partial(xz_kernel, (parts, count, nz, chunk, group)), "xz_part", me, [test] + fields, None,
        parts, count, nz, tests, group)
    partial_triad = part_call(
        partial(y_kernel, (parts, count, nz, chunk, group, scale)), "y_part", me,
        [test, next_test, running] + fields + nexts, running, parts, count, nz, tests, group)

    in_plane = scattered(partial_triad.reshape(tests, total, total), "space", 0)
    return scattered(in_plane, "mode", 1)


def solution(mesh):
    in_specs = (P(None, None, None, "space", None), P("mode", None, None, "space", None))
    return jax.shard_map(
        per_device, mesh=mesh, in_specs=in_specs, out_specs=P("space", "mode", None), check_vma=False
    )
```

```python
import math
from functools import partial

import jax
import jax.numpy as jnp
from jax import lax
from jax.experimental import pallas as pl
from jax.experimental.pallas import tpu as pltpu
from jax.sharding import PartitionSpec as P


LANES = 128
PITCH_PAD = 8
ROWS = 2
STAGES = 2


def flat_rows(field):
    count, comps, nz, rows, nx = field.shape
    tiles = nx // LANES
    split = field.reshape(count, comps, nz, rows, tiles, LANES)
    return split.transpose(0, 1, 2, 4, 3, 5).reshape(count, comps * nz * tiles * rows, LANES)


def lane_ids(count):
    return lax.broadcasted_iota(jnp.int32, (count, LANES), 1)


def spread_kernel(dims, stages, me_ref, src_ref, *refs):
    count, nz, rows, nx, chunk, parts = dims
    tiles = nx // LANES
    outs, scratch, hold, in_sems, out_sems = refs[:-4], refs[-4], refs[-3], refs[-2], refs[-1]
    depth = nz * tiles * rows
    pitch = depth + PITCH_PAD

    def arrival(a):
        target = scratch.at[a].reshape(count, pitch, LANES).at[:, pl.ds(0, depth), :]
        return pltpu.make_async_copy(src_ref.at[:, pl.ds(a * depth, depth), :], target, in_sems.at[a])

    for a in range(3):
        arrival(a).start()
    lane = lane_ids(count)
    edges = [edge_masks(lax.rem(lane + LANES - 4 * z, LANES), rows, chunk) for z in range(nz)]
    lows, highs = [low for low, _ in edges], [high for _, high in edges]

    def moved(value, amount):
        return value if amount % LANES == 0 else pltpu.roll(value, amount % LANES, 1)

    def one_comp(a, carry):
        arrival(a).wait()
        packed = [jnp.zeros((count, LANES), jnp.float32) for _ in range(parts)]
        for z in range(nz):
            lines = [
                [scratch[a, pl.ds((z * tiles + tile) * rows + y, count, stride=pitch), :] for y in range(rows)]
                for tile in range(tiles)
            ]
            for part in range(parts):
                offset = part * chunk % LANES
                value = jnp.zeros((count, LANES), jnp.float32)
                for y in range(rows):
                    mine = (lane >= y * chunk) & (lane < (y + 1) * chunk)
                    value = jnp.where(mine, moved(lines[part * chunk // LANES][y], y * chunk - offset), value)
                hold[part, z, a] = value
                after, before = (part + 1) % parts, (part - 1) % parts
                packed[after] = jnp.where(lows[z], moved(value, 4 * z - chunk), packed[after])
                packed[before] = jnp.where(highs[z], moved(value, 4 * z + chunk), packed[before])
        for part in range(parts):
            hold[part, nz, a] = packed[part]
        for copy in departures(a):
            copy.start()
        return carry

    def departures(a):
        copies = []
        for stage, (levels, halos) in enumerate(stages):
            for shift in range(parts):
                part = me_ref[0] ^ shift
                pieces = [(levels[0], len(levels), 0)] + ([(nz, 1, len(levels))] if halos else [])
                for piece, (start, size, at) in enumerate(pieces):
                    source = hold.at[part, pl.ds(start, size), a]
                    target = outs[stage * parts + shift].at[pl.ds(at, size), a]
                    copies.append(pltpu.make_async_copy(source, target, out_sems.at[a, stage * 2 + piece, shift]))
        return copies

    lax.fori_loop(0, 3, one_comp, 0)

    def finish(a, carry):
        for copy in departures(a):
            copy.wait()
        return carry

    lax.fori_loop(0, 3, finish, 0)


def edge_masks(lane, rows, chunk, width=2):
    low, high = None, None
    for y in range(rows):
        before, after = (y * chunk - width) % LANES, (y + 1) * chunk % LANES
        one = (lane >= before) & (lane < before + width)
        two = (lane >= after) & (lane < after + width)
        low, high = (one, two) if low is None else (low | one, high | two)
    return low, high


def spread(field, me, parts, stages):
    count, comps, nz, rows, nx = field.shape
    flat = flat_rows(field)
    dims = (count, nz, rows, nx, nx // parts, parts)
    shapes = [(len(levels) + (1 if halos else 0), comps, count, LANES) for levels, halos in stages for _ in range(parts)]
    outs = pl.pallas_call(
        partial(spread_kernel, dims, stages),
        out_shape=[jax.ShapeDtypeStruct(shape, jnp.float32) for shape in shapes],
        in_specs=[pl.BlockSpec(memory_space=pltpu.SMEM), pl.BlockSpec(memory_space=pl.ANY)],
        out_specs=[pl.BlockSpec(memory_space=pl.ANY) for _ in shapes],
        scratch_shapes=[
            pltpu.VMEM((comps, count * (flat.shape[1] // comps + PITCH_PAD), LANES), jnp.float32),
            pltpu.VMEM((parts, nz + 1, comps, count, LANES), jnp.float32),
            pltpu.SemaphoreType.DMA((comps,)),
            pltpu.SemaphoreType.DMA((comps, 2 * len(stages), parts)),
        ],
        compiler_params=pltpu.CompilerParams(vmem_limit_bytes=16 * 2**20),
        name="spread",
    )(me, flat)
    return [list(outs[at : at + parts]) for at in range(0, len(outs), parts)]


def own_kernel(dims, me_ref, src_ref, out_ref, scratch, sem):
    count, nz, rows, nx, chunk = dims
    tiles = nx // LANES
    depth = 3 * nz * tiles * rows
    pitch = depth + PITCH_PAD
    copy = pltpu.make_async_copy(src_ref, scratch.reshape(count, pitch, LANES).at[:, pl.ds(0, depth), :], sem)
    copy.start()
    copy.wait()
    lane = lane_ids(count)
    start = me_ref[0] * chunk
    tile, offset = start // LANES, lax.rem(start, LANES)
    for a in range(3):
        for z in range(nz):
            value = jnp.zeros((count, LANES), jnp.float32)
            for y in range(rows):
                line = scratch[pl.ds(((a * nz + z) * tiles + tile) * rows + y, count, stride=pitch), :]
                mine = (lane >= y * chunk) & (lane < (y + 1) * chunk)
                value = jnp.where(mine, pltpu.roll(line, lax.rem(y * chunk - offset + LANES, LANES), 1), value)
            out_ref[z, a] = value


def own_chunk(field, me, parts):
    count, comps, nz, rows, nx = field.shape
    flat = flat_rows(field)
    return pl.pallas_call(
        partial(own_kernel, (count, nz, rows, nx, nx // parts)),
        out_shape=jax.ShapeDtypeStruct((nz, comps, count, LANES), jnp.float32),
        in_specs=[pl.BlockSpec(memory_space=pltpu.SMEM), pl.BlockSpec(memory_space=pl.ANY)],
        scratch_shapes=[
            pltpu.VMEM((count * (flat.shape[1] + PITCH_PAD), LANES), jnp.float32),
            pltpu.SemaphoreType.DMA,
        ],
        compiler_params=pltpu.CompilerParams(vmem_limit_bytes=16 * 2**20),
        name="own_chunk",
    )(me, flat)


def split_pair(value):
    high = value.astype(jnp.bfloat16)
    return high, (value - high.astype(jnp.float32)).astype(jnp.bfloat16)


def x_grad(value, packed, z, chunk):
    lane = lane_ids(value.shape[0])
    edge = pltpu.roll(packed, LANES - 4 * z, 1) if z else packed
    diffs = []
    for width in (1, 2):
        low, high = edge_masks(lane, ROWS, chunk, width)
        ahead, behind = jnp.where(high, edge, value), jnp.where(low, edge, value)
        diffs.append(pltpu.roll(ahead, LANES - width, 1) - pltpu.roll(behind, width, 1))
    return 8.0 * diffs[0] - diffs[1]


def y_grads(own, ahead, chunk):
    first = lane_ids(own.shape[0]) < chunk

    def swapped(value):
        if 2 * chunk == LANES:
            return pltpu.roll(value, chunk, 1)
        return jnp.where(first, pltpu.roll(value, LANES - chunk, 1), pltpu.roll(value, chunk, 1))

    turned = 8.0 * swapped(own)
    mine = jnp.where(first, turned, 8.0 * swapped(ahead) - turned) - ahead
    theirs = own - jnp.where(first, turned, 0.0)
    return mine, theirs


def part_kernel(plan, steps, me_ref, *refs):
    parts, count, nz, chunk, group, span, xs, ys, zs, has_run, scale = plan
    total = parts * count
    near = {(z + step) % nz for z in zs for step in range(-2, 3)}
    stages = sorted({z // span for z in near | set(xs + ys)} | ({0} if xs else set()))
    next_stages = sorted({z // span for z in ys})
    refs = list(refs)
    test_ref = refs.pop(0)
    next_test_ref = refs.pop(0) if ys else None
    run_ref = refs.pop(0) if has_run else None
    fields = {stage: [refs.pop(0) for _ in range(parts)] for stage in stages}
    nexts = {stage: [refs.pop(0) for _ in range(parts)] for stage in next_stages}
    out_ref, grad_ref, join_ref, right_ref = refs
    slabs = [(test_ref, z) for z in xs]
    slabs += [item for z in ys for item in ((test_ref, z), (next_test_ref, z))]
    slabs += [(test_ref, z) for z in zs]

    def prepare():
        for shift in range(parts):
            at = pl.multiple_of((me_ref[0] ^ shift) * count, count)
            rows = pl.ds(at, count)

            def level(z, a):
                return fields[z // span][shift][z % span, a]

            def one_comp(a, carry):
                slab = 0
                for z in xs:
                    grad_ref[slab * 3 + a, rows, :] = x_grad(level(z, a), fields[0][shift][span, a], z, chunk)
                    slab += 1
                for z in ys:
                    mine, theirs = y_grads(level(z, a), nexts[z // span][shift][z % span, a], chunk)
                    grad_ref[slab * 3 + a, rows, :] = mine
                    grad_ref[slab * 3 + 3 + a, rows, :] = theirs
                    slab += 2
                for z in zs:
                    ahead = level((z + 1) % nz, a) - level((z - 1) % nz, a)
                    farther = level((z + 2) % nz, a) - level((z - 2) % nz, a)
                    grad_ref[slab * 3 + a, rows, :] = 8.0 * ahead - farther
                    slab += 1
                return carry

            lax.fori_loop(0, 3, one_comp, 0)
            slab = 0
            for z in xs:
                join_ref[slab, rows, :] = level(z, 0)
                slab += 1
            for z in ys:
                join_ref[slab, rows, :] = level(z, 1)
                join_ref[slab + 1, rows, :] = nexts[z // span][shift][z % span, 1]
                slab += 2
            for z in zs:
                join_ref[slab, rows, :] = level(z, 2)
                slab += 1

        def turn(slab, carry):
            high, low = split_pair(join_ref[slab].T)
            at = pl.ds(pl.multiple_of(slab * LANES, LANES), LANES)
            right_ref[at, pl.ds(0, total)] = high
            right_ref[at, pl.ds(total, total)] = low
            return carry

        lax.fori_loop(0, len(slabs), turn, 0)

    prepare()

    def one_step(step, carry):
        first = block_of(step, me_ref) * group
        dims = (((1,), (0,)), ((), ()))
        both, rest = None, None
        for start in range(0, len(slabs), 2):
            width = min(2, len(slabs) - start)
            highs, lows = [[] for _ in range(group)], [[] for _ in range(group)]
            for slab in range(start, start + width):
                source, z = slabs[slab]
                grads = [grad_ref[slab * 3 + a] for a in range(3)]
                for i in range(group):
                    tests = [source[z, a, pl.ds(first + i, 1), :] for a in range(3)]
                    high, low = split_pair(tests[0] * grads[0] + tests[1] * grads[1] + tests[2] * grads[2])
                    highs[i].append(high)
                    lows[i].append(low)
            high = jnp.concatenate([jnp.concatenate(row, 1) for row in highs], 0)
            low = jnp.concatenate([jnp.concatenate(row, 1) for row in lows], 0)
            right = right_ref[pl.ds(start * LANES, width * LANES), :]
            part = lax.dot_general(high, right, dims, preferred_element_type=jnp.float32)
            more = lax.dot_general(low, right[:, :total], dims, preferred_element_type=jnp.float32)
            both = part if both is None else both + part
            rest = more if rest is None else rest + more
        result = both[:, :total] + both[:, total:] + rest
        if has_run:
            result = result + run_ref[pl.ds(pl.multiple_of(first * total, group * total), group * total), :]
        out_ref[pl.ds(pl.multiple_of(step * group * total, group * total), group * total), :] = (
            result if scale is None else result * scale
        )
        return carry

    lax.fori_loop(0, steps, one_step, 0)


def block_of(step, me_ref):
    return me_ref[1] + me_ref[2] * (me_ref[3] ^ step)


def part_call(plan, order, steps, inputs, running=None):
    parts, count, _, _, group, _, xs, ys, zs, has_run, scale = plan
    total = parts * count
    slabs = len(xs) + 2 * len(ys) + len(zs)
    whole = pl.BlockSpec(memory_space=pltpu.VMEM)
    place = [value is running for value in inputs].index(True) + 1 if has_run and scale is None else None
    return pl.pallas_call(
        partial(part_kernel, plan, steps),
        in_specs=[pl.BlockSpec(memory_space=pltpu.SMEM)] + [whole] * len(inputs),
        out_specs=whole,
        scratch_shapes=[
            pltpu.VMEM((3 * slabs, total, LANES), jnp.float32),
            pltpu.VMEM((slabs, total, LANES), jnp.float32),
            pltpu.VMEM((slabs * LANES, 2 * total), jnp.bfloat16),
        ],
        out_shape=pltpu.VMEM((steps * group * total, total), jnp.float32)
        if place is not None or not has_run
        else jax.ShapeDtypeStruct((steps * group * total, total), jnp.float32),
        input_output_aliases={} if place is None else {place: 0},
        compiler_params=pltpu.CompilerParams(vmem_limit_bytes=16 * 2**20),
        cost_estimate=pl.CostEstimate(
            flops=6 * slabs * LANES * steps * group * total * total,
            transcendentals=0, bytes_accessed=8 * steps * group * total * total),
    )(order, *[pltpu.with_memory_space_constraint(value, pltpu.VMEM) for value in inputs])


def shifted(value, axis, shift):
    size = lax.axis_size(axis)
    return lax.ppermute(value, axis, [(i, (i + shift) % size) for i in range(size)])


def swapped_with(value, axis, other):
    return lax.ppermute(value, axis, [(i, i ^ other) for i in range(lax.axis_size(axis))])


def scattered(value, axis, dim):
    size, me = lax.axis_size(axis), lax.axis_index(axis)
    length = value.shape[dim] // size
    total = lax.dynamic_slice_in_dim(value, me * length, length, dim)
    for other in range(size - 1, 0, -1):
        block = lax.dynamic_slice_in_dim(value, (me ^ other) * length, length, dim)
        total = total + swapped_with(block, axis, other)
    return total


def per_device(test_modes, modes):
    count, _, nz, rows, nx = modes.shape
    tests = test_modes.shape[0]
    parts, slabs = lax.axis_size("mode"), lax.axis_size("space")
    chunk, group = nx // parts, tests // slabs
    assert rows == ROWS and rows * chunk <= LANES and parts & (parts - 1) == 0 and slabs & (slabs - 1) == 0 and nz % STAGES == 0
    span = nz // STAGES
    me = lax.axis_index("mode").astype(jnp.int32)
    place = lax.axis_index("space").astype(jnp.int32)
    plain = jnp.stack([me, 0, 1, 0]).astype(jnp.int32)
    scale = 1.0 / (12.0 * math.sqrt(nx * nz * rows * slabs))
    levels = [tuple(range(stage * span, (stage + 1) * span)) for stage in range(STAGES)]

    return exchange(test_modes, modes, plain, place, levels, (parts, count, nz, chunk, group, span), scale)


def exchange(test_modes, modes, plain, place, levels, dims, scale):
    parts, count, nz, _, group, span = dims
    total, slabs = parts * count, test_modes.shape[0] // group
    fields = spread(modes, plain, parts, tuple((levels[stage], stage == 0) for stage in range(STAGES)))
    for stage in range(STAGES):
        for other in range(parts - 1, 0, -1):
            fields[stage][other] = swapped_with(fields[stage][other], "mode", other)
    test = own_chunk(test_modes, plain, parts)
    next_test = shifted(test, "space", -1)
    nexts = []
    for stage in range(STAGES):
        nexts.append([shifted(field[:span], "space", -1) for field in fields[stage]])

    running = None
    for stage in range(STAGES - 1):
        for kind in ("x", "y"):
            held = fields[stage] if stage == 0 or kind == "y" else fields[0] + fields[stage]
            plan = dims + ((levels[stage], (), ()) if kind == "x" else ((), levels[stage], ()))
            plan += (running is not None, None)
            given = [test] + ([next_test] if kind == "y" else []) + ([running] if running is not None else [])
            given += held + nexts[stage] if kind == "y" else held
            running = part_call(plan, plain, slabs, given, running)
    plan = dims + (levels[-1], (), tuple(range(nz)), running is not None, None)
    given = [test] + ([running] if running is not None else []) + sum(fields, [])
    running = part_call(plan, plain, slabs, given, running)

    plan = dims + ((), levels[-1], (), True, scale)
    given = [test, next_test, running] + fields[-1] + nexts[-1]
    me = plain[0]
    chips = slabs // 2
    side, chip = place % 2, place // 2

    def last(core):
        order = jnp.stack([me, core, 2, chip]).astype(jnp.int32)
        value = part_call(plan, order, chips, given, running)
        return value.reshape(chips, group, total, total)

    other = last(1 - side)
    came = swapped_with(other, "space", 1)
    both = last(side)
    in_plane = both[0] + came[0]
    for turn in range(chips - 1, 0, -1):
        in_plane = in_plane + swapped_with(both[turn] + came[turn], "space", 2 * turn)
    return scattered(in_plane, "mode", 1)


def solution(mesh):
    in_specs = (P(None, None, None, "space", None), P("mode", None, None, "space", None))
    return jax.shard_map(
        per_device, mesh=mesh, in_specs=in_specs, out_specs=P("space", "mode", None), check_vma=False
    )
```

```python
import math
from functools import partial

import jax
import jax.numpy as jnp
from jax import lax
from jax.experimental import pallas as pl
from jax.experimental.pallas import tpu as pltpu
from jax.sharding import PartitionSpec as P


LANES = 128
PITCH_PAD = 8
ROWS = 2
STAGES = 2


def flat_rows(field):
    count, comps, nz, rows, nx = field.shape
    tiles = nx // LANES
    split = field.reshape(count, comps, nz, rows, tiles, LANES)
    return split.transpose(0, 1, 2, 4, 3, 5).reshape(count, comps * nz * tiles * rows, LANES)


def lane_ids(count):
    return lax.broadcasted_iota(jnp.int32, (count, LANES), 1)


def spread_kernel(dims, stages, me_ref, src_ref, *refs):
    count, nz, rows, nx, chunk, parts = dims
    tiles = nx // LANES
    outs, scratch, hold, in_sems = refs[:-3], refs[-3], refs[-2], refs[-1]
    depth = nz * tiles * rows
    pitch = depth + PITCH_PAD

    def arrival(a):
        target = scratch.at[a].reshape(count, pitch, LANES).at[:, pl.ds(0, depth), :]
        return pltpu.make_async_copy(src_ref.at[:, pl.ds(a * depth, depth), :], target, in_sems.at[a])

    for a in range(3):
        arrival(a).start()
    lane = lane_ids(count)
    edges = [edge_masks(lax.rem(lane + LANES - 4 * z, LANES), rows, chunk) for z in range(nz)]
    lows, highs = [low for low, _ in edges], [high for _, high in edges]

    def moved(value, amount):
        return value if amount % LANES == 0 else pltpu.roll(value, amount % LANES, 1)

    def one_comp(a, carry):
        arrival(a).wait()
        packed = [jnp.zeros((count, LANES), jnp.float32) for _ in range(parts)]
        for z in range(nz):
            lines = [
                [scratch[a, pl.ds((z * tiles + tile) * rows + y, count, stride=pitch), :] for y in range(rows)]
                for tile in range(tiles)
            ]
            for part in range(parts):
                offset = part * chunk % LANES
                value = jnp.zeros((count, LANES), jnp.float32)
                for y in range(rows):
                    mine = (lane >= y * chunk) & (lane < (y + 1) * chunk)
                    value = jnp.where(mine, moved(lines[part * chunk // LANES][y], y * chunk - offset), value)
                hold[part, z] = value
                after, before = (part + 1) % parts, (part - 1) % parts
                back = moved(value, 4 * z - chunk)
                on = back if 2 * chunk % LANES == 0 else moved(value, 4 * z + chunk)
                packed[after] = jnp.where(lows[z], back, packed[after])
                packed[before] = jnp.where(highs[z], on, packed[before])
        for part in range(parts):
            hold[part, nz] = packed[part]
        index = 0
        for levels, halos in stages:
            for shift in range(parts):
                part = me_ref[0] ^ shift
                for place, z in enumerate(levels + ((nz,) if halos else ())):
                    outs[index][place, a] = hold[part, z]
                index += 1
        return carry

    lax.fori_loop(0, 3, one_comp, 0)


def edge_masks(lane, rows, chunk):
    low, high = None, None
    for y in range(rows):
        before, after = (y * chunk - 2) % LANES, (y + 1) * chunk % LANES
        one = (lane >= before) & (lane < before + 2)
        two = (lane >= after) & (lane < after + 2)
        low, high = (one, two) if low is None else (low | one, high | two)
    return low, high


def spread(field, me, parts, stages):
    count, comps, nz, rows, nx = field.shape
    flat = flat_rows(field)
    dims = (count, nz, rows, nx, nx // parts, parts)
    shapes = [(len(levels) + (1 if halos else 0), comps, count, LANES) for levels, halos in stages for _ in range(parts)]
    outs = pl.pallas_call(
        partial(spread_kernel, dims, stages),
        out_shape=[pltpu.VMEM(shape, jnp.float32) for shape in shapes],
        in_specs=[pl.BlockSpec(memory_space=pltpu.SMEM), pl.BlockSpec(memory_space=pltpu.HBM)],
        out_specs=[pl.BlockSpec(memory_space=pltpu.VMEM) for _ in shapes],
        scratch_shapes=[
            pltpu.VMEM((comps, count * (flat.shape[1] // comps + PITCH_PAD), LANES), jnp.float32),
            pltpu.VMEM((parts, nz + 1, count, LANES), jnp.float32),
            pltpu.SemaphoreType.DMA((comps,)),
        ],
        compiler_params=pltpu.CompilerParams(vmem_limit_bytes=16 * 2**20),
        name="spread",
    )(me, pltpu.with_memory_space_constraint(flat, pltpu.HBM))
    return [list(outs[at : at + parts]) for at in range(0, len(outs), parts)]


def own_kernel(dims, me_ref, src_ref, out_ref, scratch, sem):
    count, nz, rows, nx, chunk = dims
    tiles = nx // LANES
    depth = 3 * nz * tiles * rows
    pitch = depth + PITCH_PAD
    copy = pltpu.make_async_copy(src_ref, scratch.reshape(count, pitch, LANES).at[:, pl.ds(0, depth), :], sem)
    copy.start()
    copy.wait()
    lane = lane_ids(count)
    start = me_ref[0] * chunk
    tile, offset = start // LANES, lax.rem(start, LANES)
    for a in range(3):
        for z in range(nz):
            value = jnp.zeros((count, LANES), jnp.float32)
            for y in range(rows):
                line = scratch[pl.ds(((a * nz + z) * tiles + tile) * rows + y, count, stride=pitch), :]
                mine = (lane >= y * chunk) & (lane < (y + 1) * chunk)
                value = jnp.where(mine, pltpu.roll(line, lax.rem(y * chunk - offset + LANES, LANES), 1), value)
            out_ref[z, a] = value


def own_chunk(field, me, parts):
    count, comps, nz, rows, nx = field.shape
    flat = flat_rows(field)
    return pl.pallas_call(
        partial(own_kernel, (count, nz, rows, nx, nx // parts)),
        out_shape=jax.ShapeDtypeStruct((nz, comps, count, LANES), jnp.float32),
        in_specs=[pl.BlockSpec(memory_space=pltpu.SMEM), pl.BlockSpec(memory_space=pltpu.HBM)],
        scratch_shapes=[
            pltpu.VMEM((count * (flat.shape[1] + PITCH_PAD), LANES), jnp.float32),
            pltpu.SemaphoreType.DMA,
        ],
        compiler_params=pltpu.CompilerParams(vmem_limit_bytes=16 * 2**20),
        name="own_chunk",
    )(me, pltpu.with_memory_space_constraint(flat, pltpu.HBM))


def split_pair(value):
    high = value.astype(jnp.bfloat16)
    return high, (value - high.astype(jnp.float32)).astype(jnp.bfloat16)


def x_band(z, chunk):
    row = lax.broadcasted_iota(jnp.int32, (LANES, LANES), 0)
    column = lax.broadcasted_iota(jnp.int32, (LANES, LANES), 1)
    bands = []
    for source, inside in ((row, True), (lax.rem(row + LANES - 4 * z, LANES), False)):
        gap = lax.rem(source - column + LANES + LANES // 2, LANES) - LANES // 2
        near = jnp.where(gap == 1, 8.0, jnp.where(gap == -1, -8.0, 0.0))
        band = jnp.where(gap == 2, -1.0, jnp.where(gap == -2, 1.0, near))
        same = source // chunk == column // chunk
        bands.append(jnp.where(same if inside else ~same, band, 0.0))
    return jnp.concatenate(bands, 0).astype(jnp.bfloat16)


def x_grads(values, packed, z, chunk):
    band = x_band(z, chunk)
    total = None
    for piece in zip(split_pair(values), split_pair(packed)):
        part = lax.dot_general(
            jnp.concatenate(piece, 1), band, (((1,), (0,)), ((), ())), preferred_element_type=jnp.float32
        )
        total = part if total is None else total + part
    return total


def y_grads(own, ahead, chunk):
    first = lane_ids(own.shape[0]) < chunk

    def swapped(value):
        if 2 * chunk == LANES:
            return pltpu.roll(value, chunk, 1)
        return jnp.where(first, pltpu.roll(value, LANES - chunk, 1), pltpu.roll(value, chunk, 1))

    turned = 8.0 * swapped(own)
    mine = jnp.where(first, turned, 8.0 * swapped(ahead) - turned) - ahead
    theirs = own - jnp.where(first, turned, 0.0)
    return mine, theirs


def part_kernel(plan, steps, me_ref, *refs):
    parts, count, nz, chunk, group, span, xs, ys, zs, has_run, scale, tables = plan
    total = parts * count
    near = {(z + step) % nz for z in zs for step in range(-2, 3)}
    stages = sorted({z // span for z in near | set(xs + ys)} | ({0} if xs else set()))
    next_stages = sorted({z // span for z in ys})
    refs = list(refs)
    test_ref = refs.pop(0)
    next_test_ref = refs.pop(0) if ys else None
    run_ref = refs.pop(0) if has_run else None
    if tables != "given":
        fields = {stage: [refs.pop(0) for _ in range(parts)] for stage in stages}
        nexts = {stage: [refs.pop(0) for _ in range(parts)] for stage in next_stages}
    if tables == "keep":
        out_ref, grad_ref, right_ref, join_ref = refs
    elif tables == "given":
        grad_ref, right_ref, out_ref = refs
    else:
        out_ref, grad_ref, join_ref, right_ref = refs
    slabs = [(test_ref, z) for z in xs]
    slabs += [item for z in ys for item in ((test_ref, z), (next_test_ref, z))]
    slabs += [(test_ref, z) for z in zs]

    def place(shift):
        return pl.ds(pl.multiple_of((me_ref[0] ^ shift) * count, count), count)

    def prepare_x():
        packed = jnp.concatenate([fields[0][shift][span].reshape(3 * count, LANES) for shift in range(parts)], 0)
        for slab, z in enumerate(xs):
            values = [fields[z // span][shift][z % span].reshape(3 * count, LANES) for shift in range(parts)]
            grads = x_grads(jnp.concatenate(values, 0), packed, z, chunk)
            for shift in range(parts):
                for a in range(3):
                    at = (shift * 3 + a) * count
                    grad_ref[slab * 3 + a, place(shift), :] = grads[at : at + count]

    def prepare():
        if xs:
            prepare_x()
        for shift in range(parts):
            rows = place(shift)

            def level(z, a):
                return fields[z // span][shift][z % span, a]

            def one_comp(a, carry):
                slab = len(xs)
                for z in ys:
                    mine, theirs = y_grads(level(z, a), nexts[z // span][shift][z % span, a], chunk)
                    grad_ref[slab * 3 + a, rows, :] = mine
                    grad_ref[slab * 3 + 3 + a, rows, :] = theirs
                    slab += 2
                for z in zs:
                    ahead = level((z + 1) % nz, a) - level((z - 1) % nz, a)
                    farther = level((z + 2) % nz, a) - level((z - 2) % nz, a)
                    grad_ref[slab * 3 + a, rows, :] = 8.0 * ahead - farther
                    slab += 1
                return carry

            if ys or zs:
                lax.fori_loop(0, 3, one_comp, 0)
            slab = 0
            for z in xs:
                join_ref[slab, rows, :] = level(z, 0)
                slab += 1
            for z in ys:
                join_ref[slab, rows, :] = level(z, 1)
                join_ref[slab + 1, rows, :] = nexts[z // span][shift][z % span, 1]
                slab += 2
            for z in zs:
                join_ref[slab, rows, :] = level(z, 2)
                slab += 1

        def turn(slab, carry):
            high, low = split_pair(join_ref[slab].T)
            at = pl.ds(pl.multiple_of(slab * LANES, LANES), LANES)
            right_ref[at, pl.ds(0, total)] = high
            right_ref[at, pl.ds(total, total)] = low
            return carry

        lax.fori_loop(0, len(slabs), turn, 0)

    if tables != "given":
        prepare()

    def one_step(step, carry):
        first = block_of(step, me_ref) * group
        dims = (((1,), (0,)), ((), ()))
        both, rest = None, None
        for start in range(0, len(slabs), 2):
            width = min(2, len(slabs) - start)
            highs, lows = [[] for _ in range(group)], [[] for _ in range(group)]
            for slab in range(start, start + width):
                source, z = slabs[slab]
                grads = [grad_ref[slab * 3 + a] for a in range(3)]
                for i in range(group):
                    tests = [source[z, a, pl.ds(first + i, 1), :] for a in range(3)]
                    high, low = split_pair(tests[0] * grads[0] + tests[1] * grads[1] + tests[2] * grads[2])
                    highs[i].append(high)
                    lows[i].append(low)
            high = jnp.concatenate([jnp.concatenate(row, 1) for row in highs], 0)
            low = jnp.concatenate([jnp.concatenate(row, 1) for row in lows], 0)
            right = right_ref[pl.ds(start * LANES, width * LANES), :]
            part = lax.dot_general(high, right, dims, preferred_element_type=jnp.float32)
            more = lax.dot_general(low, right[:, :total], dims, preferred_element_type=jnp.float32)
            both = part if both is None else both + part
            rest = more if rest is None else rest + more
        result = both[:, :total] + both[:, total:] + rest
        if has_run:
            result = result + run_ref[pl.ds(pl.multiple_of(first * total, group * total), group * total), :]
        out_ref[pl.ds(pl.multiple_of(step * group * total, group * total), group * total), :] = (
            result if scale is None else result * scale
        )
        return carry

    lax.fori_loop(0, steps, one_step, 0, unroll=2)


def block_of(step, me_ref):
    return me_ref[1] + me_ref[2] * (me_ref[3] ^ step)


def part_call(plan, order, steps, inputs, running=None):
    parts, count, _, _, group, _, xs, ys, zs, has_run, scale, tables = plan
    total = parts * count
    slabs = len(xs) + 2 * len(ys) + len(zs)
    whole = pl.BlockSpec(memory_space=pltpu.VMEM)
    place = [value is running for value in inputs].index(True) + 1 if has_run and scale is None else None
    out = pltpu.VMEM((steps * group * total, total), jnp.float32)
    grads = pltpu.VMEM((3 * slabs, total, LANES), jnp.float32)
    joined = pltpu.VMEM((slabs, total, LANES), jnp.float32)
    rights = pltpu.VMEM((slabs * LANES, 2 * total), jnp.bfloat16)
    outs, scratch = {"": ([out], [grads, joined, rights]), "keep": ([out, grads, rights], [joined]), "given": ([out], [])}[tables]
    return pl.pallas_call(
        partial(part_kernel, plan, steps),
        in_specs=[pl.BlockSpec(memory_space=pltpu.SMEM)] + [whole] * len(inputs),
        out_specs=[whole] * len(outs),
        out_shape=outs,
        scratch_shapes=scratch,
        input_output_aliases={} if place is None else {place: 0},
        compiler_params=pltpu.CompilerParams(vmem_limit_bytes=16 * 2**20),
        cost_estimate=pl.CostEstimate(
            flops=6 * slabs * LANES * steps * group * total * total,
            transcendentals=0, bytes_accessed=8 * steps * group * total * total),
    )(order, *[pltpu.with_memory_space_constraint(value, pltpu.VMEM) for value in inputs])


def shifted(value, axis, shift):
    size = lax.axis_size(axis)
    return lax.ppermute(value, axis, [(i, (i + shift) % size) for i in range(size)])


def swapped_with(value, axis, other):
    return lax.ppermute(value, axis, [(i, i ^ other) for i in range(lax.axis_size(axis))])


def scattered(value, axis, dim):
    size, me = lax.axis_size(axis), lax.axis_index(axis)
    length = value.shape[dim] // size
    total = lax.dynamic_slice_in_dim(value, me * length, length, dim)
    for other in range(size - 1, 0, -1):
        block = lax.dynamic_slice_in_dim(value, (me ^ other) * length, length, dim)
        total = total + swapped_with(block, axis, other)
    return total


def per_device(test_modes, modes):
    count, _, nz, rows, nx = modes.shape
    tests = test_modes.shape[0]
    parts, slabs = lax.axis_size("mode"), lax.axis_size("space")
    chunk, group = nx // parts, tests // slabs
    assert rows == ROWS and rows * chunk <= LANES and parts & (parts - 1) == 0 and slabs & (slabs - 1) == 0 and nz % STAGES == 0
    span = nz // STAGES
    me = lax.axis_index("mode").astype(jnp.int32)
    place = lax.axis_index("space").astype(jnp.int32)
    plain = jnp.stack([me, 0, 1, 0]).astype(jnp.int32)
    scale = 1.0 / (12.0 * math.sqrt(nx * nz * rows * slabs))
    levels = [tuple(range(stage * span, (stage + 1) * span)) for stage in range(STAGES)]

    return exchange(test_modes, modes, plain, place, levels, (parts, count, nz, chunk, group, span), scale)


def exchange(test_modes, modes, plain, place, levels, dims, scale):
    parts, count, nz, _, group, span = dims
    total, slabs = parts * count, test_modes.shape[0] // group
    fields = spread(modes, plain, parts, tuple((levels[stage], stage == 0) for stage in range(STAGES)))
    for stage in range(STAGES):
        for other in range(parts - 1, 0, -1):
            fields[stage][other] = swapped_with(fields[stage][other], "mode", other)
    test = own_chunk(test_modes, plain, parts)
    next_test = shifted(test, "space", -1)
    nexts = []
    for stage in range(STAGES):
        nexts.append([shifted(field[:span], "space", -1) for field in fields[stage]])

    running = None
    for stage in range(STAGES - 1):
        for kind in ("x", "y"):
            held = fields[stage] if stage == 0 or kind == "y" else fields[0] + fields[stage]
            plan = dims + ((levels[stage], (), ()) if kind == "x" else ((), levels[stage], ()))
            plan += (running is not None, None, "")
            given = [test] + ([next_test] if kind == "y" else []) + ([running] if running is not None else [])
            given += held + nexts[stage] if kind == "y" else held
            running = part_call(plan, plain, slabs, given, running)[0]
    plan = dims + (levels[-1], (), tuple(range(nz)), running is not None, None, "")
    given = [test] + ([running] if running is not None else []) + sum(fields, [])
    running = part_call(plan, plain, slabs, given, running)[0]

    me = plain[0]
    side, chip, half = place % 2, place // 2, slabs // 4

    def last(core, start, steps, tables, given):
        plan = dims + ((), levels[-1], (), True, scale, tables)
        order = jnp.stack([me, core, 2, start]).astype(jnp.int32)
        value, *held = part_call(plan, order, steps, [test, next_test, running] + given, running)
        return value.reshape(steps, group, total, total), held

    far_start = chip ^ half
    value, held = last(1 - side, far_start, half, "keep", fields[-1] + nexts[-1])
    far_came = swapped_with(value, "space", 1)
    value, _ = last(1 - side, chip, half, "given", held)
    came = swapped_with(value, "space", 1)
    far, _ = last(side, far_start, half, "given", held)
    sent = [None] * half
    for step in range(half - 1, -1, -1):
        sent[step] = swapped_with(far[step] + far_came[step], "space", 2 * (half + step))
    near, _ = last(side, chip, half, "given", held)
    in_plane = near[0] + came[0]
    for step in range(half - 1, 0, -1):
        in_plane = in_plane + swapped_with(near[step] + came[step], "space", 2 * step)
    for value in sent:
        in_plane = in_plane + value
    return scattered(in_plane, "mode", 1)


def solution(mesh):
    in_specs = (P(None, None, None, "space", None), P("mode", None, None, "space", None))
    return jax.shard_map(
        per_device, mesh=mesh, in_specs=in_specs, out_specs=P("space", "mode", None), check_vma=False
    )
```

```python
import math
from functools import partial

import jax
import jax.numpy as jnp
from jax import lax
from jax.experimental import pallas as pl
from jax.experimental.pallas import tpu as pltpu
from jax.sharding import PartitionSpec as P


LANES = 128
PITCH_PAD = 8
ROWS = 2
STAGES = 2


def flat_rows(field):
    count, comps, nz, rows, nx = field.shape
    tiles = nx // LANES
    split = field.reshape(count, comps, nz, rows, tiles, LANES)
    return split.transpose(0, 1, 2, 4, 3, 5).reshape(count, comps * nz * tiles * rows, LANES)


def lane_ids(count):
    return lax.broadcasted_iota(jnp.int32, (count, LANES), 1)


def spread_kernel(dims, stages, me_ref, src_ref, *refs):
    count, nz, rows, nx, chunk, parts = dims
    tiles = nx // LANES
    outs, scratch, hold, in_sems = refs[:-3], refs[-3], refs[-2], refs[-1]
    edged = any(halos for _, halos in stages)
    depth = nz * tiles * rows
    pitch = depth + PITCH_PAD

    def arrival(a):
        target = scratch.at[a].reshape(count, pitch, LANES).at[:, pl.ds(0, depth), :]
        return pltpu.make_async_copy(src_ref.at[:, pl.ds(a * depth, depth), :], target, in_sems.at[a])

    for a in range(3):
        arrival(a).start()
    lane = lane_ids(count)
    edges = [edge_masks(lax.rem(lane + LANES - 4 * z, LANES), rows, chunk) for z in range(nz)]
    lows, highs = [low for low, _ in edges], [high for _, high in edges]

    def moved(value, amount):
        return value if amount % LANES == 0 else pltpu.roll(value, amount % LANES, 1)

    def one_comp(a, carry):
        arrival(a).wait()
        packed = [jnp.zeros((count, LANES), jnp.float32) for _ in range(parts)]
        for z in range(nz):
            lines = [
                [scratch[a, pl.ds((z * tiles + tile) * rows + y, count, stride=pitch), :] for y in range(rows)]
                for tile in range(tiles)
            ]
            for part in range(parts):
                offset = part * chunk % LANES
                value = jnp.zeros((count, LANES), jnp.float32)
                for y in range(rows):
                    mine = (lane >= y * chunk) & (lane < (y + 1) * chunk)
                    value = jnp.where(mine, moved(lines[part * chunk // LANES][y], y * chunk - offset), value)
                hold[part, z] = value
                after, before = (part + 1) % parts, (part - 1) % parts
                if not edged:
                    continue
                back = moved(value, 4 * z - chunk)
                on = back if 2 * chunk % LANES == 0 else moved(value, 4 * z + chunk)
                packed[after] = jnp.where(lows[z], back, packed[after])
                packed[before] = jnp.where(highs[z], on, packed[before])
        for part in range(parts):
            hold[part, nz] = packed[part]
        index = 0
        for levels, halos in stages:
            for shift in range(parts):
                part = me_ref[0] ^ shift
                for place, z in enumerate(levels + ((nz,) if halos else ())):
                    outs[index][place, a] = hold[part, z]
                index += 1
        return carry

    lax.fori_loop(0, 3, one_comp, 0)


def edge_masks(lane, rows, chunk):
    low, high = None, None
    for y in range(rows):
        before, after = (y * chunk - 2) % LANES, (y + 1) * chunk % LANES
        one = (lane >= before) & (lane < before + 2)
        two = (lane >= after) & (lane < after + 2)
        low, high = (one, two) if low is None else (low | one, high | two)
    return low, high


def spread(field, me, parts, stages):
    count, comps, nz, rows, nx = field.shape
    flat = flat_rows(field)
    dims = (count, nz, rows, nx, nx // parts, parts)
    shapes = [(len(levels) + (1 if halos else 0), comps, count, LANES) for levels, halos in stages for _ in range(parts)]
    outs = pl.pallas_call(
        partial(spread_kernel, dims, stages),
        out_shape=[pltpu.VMEM(shape, jnp.float32) for shape in shapes],
        in_specs=[pl.BlockSpec(memory_space=pltpu.SMEM), pl.BlockSpec(memory_space=pltpu.HBM)],
        out_specs=[pl.BlockSpec(memory_space=pltpu.VMEM) for _ in shapes],
        scratch_shapes=[
            pltpu.VMEM((comps, count * (flat.shape[1] // comps + PITCH_PAD), LANES), jnp.float32),
            pltpu.VMEM((parts, nz + 1, count, LANES), jnp.float32),
            pltpu.SemaphoreType.DMA((comps,)),
        ],
        compiler_params=pltpu.CompilerParams(vmem_limit_bytes=16 * 2**20),
        name="spread",
    )(me, pltpu.with_memory_space_constraint(flat, pltpu.HBM))
    return [list(outs[at : at + parts]) for at in range(0, len(outs), parts)]


def own_kernel(dims, me_ref, src_ref, out_ref, scratch, sem):
    count, nz, rows, nx, chunk = dims
    tiles = nx // LANES
    depth = 3 * nz * tiles * rows
    pitch = depth + PITCH_PAD
    copy = pltpu.make_async_copy(src_ref, scratch.reshape(count, pitch, LANES).at[:, pl.ds(0, depth), :], sem)
    copy.start()
    copy.wait()
    lane = lane_ids(count)
    start = me_ref[0] * chunk
    tile, offset = start // LANES, lax.rem(start, LANES)
    for a in range(3):
        for z in range(nz):
            value = jnp.zeros((count, LANES), jnp.float32)
            for y in range(rows):
                line = scratch[pl.ds(((a * nz + z) * tiles + tile) * rows + y, count, stride=pitch), :]
                mine = (lane >= y * chunk) & (lane < (y + 1) * chunk)
                value = jnp.where(mine, pltpu.roll(line, lax.rem(y * chunk - offset + LANES, LANES), 1), value)
            out_ref[z, a] = value


def own_chunk(field, me, parts):
    count, comps, nz, rows, nx = field.shape
    flat = flat_rows(field)
    return pl.pallas_call(
        partial(own_kernel, (count, nz, rows, nx, nx // parts)),
        out_shape=jax.ShapeDtypeStruct((nz, comps, count, LANES), jnp.float32),
        in_specs=[pl.BlockSpec(memory_space=pltpu.SMEM), pl.BlockSpec(memory_space=pltpu.HBM)],
        scratch_shapes=[
            pltpu.VMEM((count * (flat.shape[1] + PITCH_PAD), LANES), jnp.float32),
            pltpu.SemaphoreType.DMA,
        ],
        compiler_params=pltpu.CompilerParams(vmem_limit_bytes=16 * 2**20),
        name="own_chunk",
    )(me, pltpu.with_memory_space_constraint(flat, pltpu.HBM))


def split_pair(value):
    high = value.astype(jnp.bfloat16)
    return high, (value - high.astype(jnp.float32)).astype(jnp.bfloat16)


def x_band(z, chunk):
    row = lax.broadcasted_iota(jnp.int32, (LANES, LANES), 0)
    column = lax.broadcasted_iota(jnp.int32, (LANES, LANES), 1)
    bands = []
    for source, inside in ((row, True), (lax.rem(row + LANES - 4 * z, LANES), False)):
        gap = lax.rem(source - column + LANES + LANES // 2, LANES) - LANES // 2
        near = jnp.where(gap == 1, 8.0, jnp.where(gap == -1, -8.0, 0.0))
        band = jnp.where(gap == 2, -1.0, jnp.where(gap == -2, 1.0, near))
        same = source // chunk == column // chunk
        bands.append(jnp.where(same if inside else ~same, band, 0.0))
    return jnp.concatenate(bands, 0).astype(jnp.bfloat16)


def x_grads(values, packed, z, chunk):
    band = x_band(z, chunk)
    total = None
    for piece in zip(split_pair(values), split_pair(packed)):
        part = lax.dot_general(
            jnp.concatenate(piece, 1), band, (((1,), (0,)), ((), ())), preferred_element_type=jnp.float32
        )
        total = part if total is None else total + part
    return total


def y_grads(own, ahead, chunk):
    first = lane_ids(own.shape[0]) < chunk

    def swapped(value):
        if 2 * chunk == LANES:
            return pltpu.roll(value, chunk, 1)
        return jnp.where(first, pltpu.roll(value, LANES - chunk, 1), pltpu.roll(value, chunk, 1))

    turned = 8.0 * swapped(own)
    mine = jnp.where(first, turned, 8.0 * swapped(ahead) - turned) - ahead
    theirs = own - jnp.where(first, turned, 0.0)
    return mine, theirs


def part_kernel(plan, steps, me_ref, *refs):
    parts, count, nz, chunk, group, span, xs, ys, zs, has_run, scale, tables = plan
    total = parts * count
    near = {(z + step) % nz for z in zs for step in range(-2, 3)}
    stages = sorted({z // span for z in near | set(xs + ys)})
    next_stages = sorted({z // span for z in ys})
    refs = list(refs)
    test_ref = refs.pop(0)
    next_test_ref = refs.pop(0) if ys else None
    run_ref = refs.pop(0) if has_run else None
    if tables != "given":
        edges = [refs.pop(0) for _ in range(parts)] if xs else None
        fields = {stage: [refs.pop(0) for _ in range(parts)] for stage in stages}
        nexts = {stage: [refs.pop(0) for _ in range(parts)] for stage in next_stages}
    if tables == "keep":
        out_ref, grad_ref, right_ref, join_ref = refs
    elif tables == "given":
        grad_ref, right_ref, out_ref = refs
    else:
        out_ref, grad_ref, join_ref, right_ref = refs
    slabs = [(test_ref, z) for z in xs]
    slabs += [item for z in ys for item in ((test_ref, z), (next_test_ref, z))]
    slabs += [(test_ref, z) for z in zs]

    def place(shift):
        return pl.ds(pl.multiple_of((me_ref[0] ^ shift) * count, count), count)

    def prepare_x():
        packed = jnp.concatenate([edges[shift][0].reshape(3 * count, LANES) for shift in range(parts)], 0)
        for slab, z in enumerate(xs):
            values = [fields[z // span][shift][z % span].reshape(3 * count, LANES) for shift in range(parts)]
            grads = x_grads(jnp.concatenate(values, 0), packed, z, chunk)
            for shift in range(parts):
                for a in range(3):
                    at = (shift * 3 + a) * count
                    grad_ref[slab * 3 + a, place(shift), :] = grads[at : at + count]

    def prepare():
        if xs:
            prepare_x()
        for shift in range(parts):
            rows = place(shift)

            def level(z, a):
                return fields[z // span][shift][z % span, a]

            def one_comp(a, carry):
                slab = len(xs)
                for z in ys:
                    mine, theirs = y_grads(level(z, a), nexts[z // span][shift][z % span, a], chunk)
                    grad_ref[slab * 3 + a, rows, :] = mine
                    grad_ref[slab * 3 + 3 + a, rows, :] = theirs
                    slab += 2
                for z in zs:
                    ahead = level((z + 1) % nz, a) - level((z - 1) % nz, a)
                    farther = level((z + 2) % nz, a) - level((z - 2) % nz, a)
                    grad_ref[slab * 3 + a, rows, :] = 8.0 * ahead - farther
                    slab += 1
                return carry

            if ys or zs:
                lax.fori_loop(0, 3, one_comp, 0)
            slab = 0
            for z in xs:
                join_ref[slab, rows, :] = level(z, 0)
                slab += 1
            for z in ys:
                join_ref[slab, rows, :] = level(z, 1)
                join_ref[slab + 1, rows, :] = nexts[z // span][shift][z % span, 1]
                slab += 2
            for z in zs:
                join_ref[slab, rows, :] = level(z, 2)
                slab += 1

        def turn(slab, carry):
            high, low = split_pair(join_ref[slab].T)
            at = pl.ds(pl.multiple_of(slab * LANES, LANES), LANES)
            right_ref[at, pl.ds(0, total)] = high
            right_ref[at, pl.ds(total, total)] = low
            return carry

        lax.fori_loop(0, len(slabs), turn, 0)

    if tables != "given":
        prepare()

    def one_step(step, carry):
        first = block_of(step, me_ref) * group
        dims = (((1,), (0,)), ((), ()))
        both, rest = None, None
        for start in range(0, len(slabs), 2):
            width = min(2, len(slabs) - start)
            highs, lows = [[] for _ in range(group)], [[] for _ in range(group)]
            for slab in range(start, start + width):
                source, z = slabs[slab]
                grads = [grad_ref[slab * 3 + a] for a in range(3)]
                for i in range(group):
                    tests = [source[z, a, pl.ds(first + i, 1), :] for a in range(3)]
                    high, low = split_pair(tests[0] * grads[0] + tests[1] * grads[1] + tests[2] * grads[2])
                    highs[i].append(high)
                    lows[i].append(low)
            high = jnp.concatenate([jnp.concatenate(row, 1) for row in highs], 0)
            low = jnp.concatenate([jnp.concatenate(row, 1) for row in lows], 0)
            right = right_ref[pl.ds(start * LANES, width * LANES), :]
            part = lax.dot_general(high, right, dims, preferred_element_type=jnp.float32)
            more = lax.dot_general(low, right[:, :total], dims, preferred_element_type=jnp.float32)
            both = part if both is None else both + part
            rest = more if rest is None else rest + more
        result = both[:, :total] + both[:, total:] + rest
        if has_run:
            result = result + run_ref[pl.ds(pl.multiple_of(first * total, group * total), group * total), :]
        out_ref[pl.ds(pl.multiple_of(step * group * total, group * total), group * total), :] = (
            result if scale is None else result * scale
        )
        return carry

    lax.fori_loop(0, steps, one_step, 0, unroll=2)


def block_of(step, me_ref):
    return me_ref[1] + me_ref[2] * (me_ref[3] ^ step)


def part_call(plan, order, steps, inputs, running=None):
    parts, count, _, _, group, _, xs, ys, zs, has_run, scale, tables = plan
    total = parts * count
    slabs = len(xs) + 2 * len(ys) + len(zs)
    whole = pl.BlockSpec(memory_space=pltpu.VMEM)
    place = [value is running for value in inputs].index(True) + 1 if has_run and scale is None else None
    out = pltpu.VMEM((steps * group * total, total), jnp.float32)
    grads = pltpu.VMEM((3 * slabs, total, LANES), jnp.float32)
    joined = pltpu.VMEM((slabs, total, LANES), jnp.float32)
    rights = pltpu.VMEM((slabs * LANES, 2 * total), jnp.bfloat16)
    outs, scratch = {"": ([out], [grads, joined, rights]), "keep": ([out, grads, rights], [joined]), "given": ([out], [])}[tables]
    return pl.pallas_call(
        partial(part_kernel, plan, steps),
        in_specs=[pl.BlockSpec(memory_space=pltpu.SMEM)] + [whole] * len(inputs),
        out_specs=[whole] * len(outs),
        out_shape=outs,
        scratch_shapes=scratch,
        input_output_aliases={} if place is None else {place: 0},
        compiler_params=pltpu.CompilerParams(vmem_limit_bytes=16 * 2**20),
        cost_estimate=pl.CostEstimate(
            flops=6 * slabs * LANES * steps * group * total * total,
            transcendentals=0, bytes_accessed=8 * steps * group * total * total),
    )(order, *[pltpu.with_memory_space_constraint(value, pltpu.VMEM) for value in inputs])


def shifted(value, axis, shift):
    size = lax.axis_size(axis)
    return lax.ppermute(value, axis, [(i, (i + shift) % size) for i in range(size)])


def swapped_with(value, axis, other):
    return lax.ppermute(value, axis, [(i, i ^ other) for i in range(lax.axis_size(axis))])


def scattered(value, axis, dim):
    size, me = lax.axis_size(axis), lax.axis_index(axis)
    length = value.shape[dim] // size
    total = lax.dynamic_slice_in_dim(value, me * length, length, dim)
    for other in range(size - 1, 0, -1):
        block = lax.dynamic_slice_in_dim(value, (me ^ other) * length, length, dim)
        total = total + swapped_with(block, axis, other)
    return total


def per_device(test_modes, modes):
    count, _, nz, rows, nx = modes.shape
    tests = test_modes.shape[0]
    parts, slabs = lax.axis_size("mode"), lax.axis_size("space")
    chunk, group = nx // parts, tests // slabs
    assert rows == ROWS and rows * chunk <= LANES and parts & (parts - 1) == 0 and slabs & (slabs - 1) == 0 and nz % STAGES == 0
    span = nz // STAGES
    me = lax.axis_index("mode").astype(jnp.int32)
    place = lax.axis_index("space").astype(jnp.int32)
    plain = jnp.stack([me, 0, 1, 0]).astype(jnp.int32)
    scale = 1.0 / (12.0 * math.sqrt(nx * nz * rows * slabs))
    levels = [tuple(range(stage * span, (stage + 1) * span)) for stage in range(STAGES)]

    return exchange(test_modes, modes, plain, place, levels, (parts, count, nz, chunk, group, span), scale)


def exchange(test_modes, modes, plain, place, levels, dims, scale):
    parts, count, nz, _, group, span = dims
    total, slabs = parts * count, test_modes.shape[0] // group
    fields = spread(modes, plain, parts, tuple((levels[stage], False) for stage in range(STAGES)))
    for stage in range(STAGES):
        for other in range(parts - 1, 0, -1):
            fields[stage][other] = swapped_with(fields[stage][other], "mode", other)
    edges = spread(modes, plain, parts, (((), True),))[0]
    for other in range(parts - 1, 0, -1):
        edges[other] = swapped_with(edges[other], "mode", other)
    test = own_chunk(test_modes, plain, parts)
    next_test = shifted(test, "space", -1)
    nexts = []
    for stage in range(STAGES):
        nexts.append([shifted(field[:span], "space", -1) for field in fields[stage]])

    running = None
    for stage in range(STAGES - 1):
        for kind in ("x", "y"):
            held = fields[stage]
            plan = dims + ((levels[stage], (), ()) if kind == "x" else ((), levels[stage], ()))
            plan += (running is not None, None, "")
            given = [test] + ([next_test] if kind == "y" else []) + ([running] if running is not None else [])
            given += held + nexts[stage] if kind == "y" else edges + held
            running = part_call(plan, plain, slabs, given, running)[0]
    plan = dims + (levels[-1], (), tuple(range(nz)), running is not None, None, "")
    given = [test] + ([running] if running is not None else []) + edges + sum(fields, [])
    running = part_call(plan, plain, slabs, given, running)[0]

    me = plain[0]
    side, chip, half = place % 2, place // 2, slabs // 4

    def last(core, start, steps, tables, given):
        plan = dims + ((), levels[-1], (), True, scale, tables)
        order = jnp.stack([me, core, 2, start]).astype(jnp.int32)
        value, *held = part_call(plan, order, steps, [test, next_test, running] + given, running)
        return value.reshape(steps, group, total, total), held

    far_start = chip ^ half
    value, held = last(1 - side, far_start, half, "keep", fields[-1] + nexts[-1])
    far_came = swapped_with(value, "space", 1)
    value, _ = last(1 - side, chip, half, "given", held)
    came = swapped_with(value, "space", 1)
    far, _ = last(side, far_start, half, "given", held)
    sent = [None] * half
    for step in range(half - 1, -1, -1):
        sent[step] = swapped_with(far[step] + far_came[step], "space", 2 * (half + step))
    near, _ = last(side, chip, half, "given", held)
    in_plane = near[0] + came[0]
    for step in range(half - 1, 0, -1):
        in_plane = in_plane + swapped_with(near[step] + came[step], "space", 2 * step)
    for value in sent:
        in_plane = in_plane + value
    return scattered(in_plane, "mode", 1)


def solution(mesh):
    in_specs = (P(None, None, None, "space", None), P("mode", None, None, "space", None))
    return jax.shard_map(
        per_device, mesh=mesh, in_specs=in_specs, out_specs=P("space", "mode", None), check_vma=False
    )
```
